512 devices in a mesh: rows: 128 (over z, y, x_lo), feat: 4 (over x_hi, core).
Axes of the slice: x: 4 (x_hi: 2, x_lo: 2; x = x_hi * 2 + x_lo), y: 8, z: 8, core: 2. Of those that a mesh axis runs over, the one named last changes fastest.
Arguments:
- bin_index: int32 [262144, 512], P('rows', 'feat'), may hold values from 0 to 255
- leaf_ids: int32 [262144], P('rows'), may hold values from 0 to 15
- gradients: bfloat16 [262144], P('rows'), may hold values from -3 to 3
- hessians: bfloat16 [262144], P('rows'), may hold values from 0.049804688 to 0.25
Outputs:
- split_gains: float32 [4, 128, 16, 256], P('feat', 'rows')
- best_gain: float32 [16], replicated
The draws below stay inside these ranges and needn't reach their ends.
All inputs are finite; a program needn't handle non-finite values.
Results may differ from the reference program's by a relative error of at most 0.0003.
Values may be sent and summed in bfloat16 or wider, within the bound.
A program may use at most 64 MiB of HBM per device.

```python
import math
import jax
import jax.numpy as jnp
import numpy as np
from jax import lax

FEATURES = 512
BINS = 256
LEAVES = 16
ROW_TOTAL = 262144
N_FEAT = 4


def touch_ends(entries, rng, low, high):
    longest = entries.shape.index(max(entries.shape))
    spots = []
    for shift in (0, 1):
        where = [jax.random.randint(jax.random.fold_in(rng, axis), (), 0, length) for axis, length in enumerate(entries.shape)]
        where[longest] = (where[longest] + shift) % entries.shape[longest]
        spots.append(tuple(where))
    return entries.at[spots[0]].set(low).at[spots[1]].set(high)


def block_levels(key, extent, cuts, low, top_value):
    factor_of, own = 1.0, jax.random.fold_in(key, 6)
    for position, shards_of in cuts:
        steps = jnp.exp(jax.random.uniform(jax.random.fold_in(own, position), (shards_of,), jnp.float32, low / len(cuts), top_value / len(cuts)))
        factor_of = factor_of * jnp.repeat(steps, extent[position] // shards_of).reshape([-1 if axis == position else 1 for axis in range(len(extent))])
    return factor_of


def cumulative_ranks(number_of, lean):
    loads = [(1 << 20) // math.isqrt(standing ** lean) + 1 for standing in range(1, number_of + 1)]
    width = 1 + sum(loads) // (1 << 30)
    return np.cumsum(np.array([max(1, weight // width) for weight in loads]))


def skewed_ids(own_key, shape, amount, lean):
    grid = cumulative_ranks(amount, lean)
    pick = jax.random.randint(jax.random.fold_in(own_key, 1), shape, 0, int(grid[amount - 1]))
    standing = jnp.searchsorted(jnp.asarray(grid, jnp.int32), pick, side="right")
    return jax.random.permutation(jax.random.fold_in(own_key, 2), amount)[standing].astype(jnp.int32)


def noise(stream_key, shape, spread, most, split=(), kind=jnp.bfloat16):
    loudness = block_levels(stream_key, shape, split, -0.22, 0.18) if split else 1.0
    result = jax.random.normal(stream_key, shape, jnp.float32) * spread * loudness
    return jnp.minimum(jnp.maximum(result, -most), most).astype(kind)


def setup_inputs(seed: int = 0) -> dict:
    arg_keys = jax.random.split(jax.random.key(seed), 5)
    return {
        "bin_index": touch_ends(jax.random.randint(arg_keys[0], (ROW_TOTAL, FEATURES), 0, BINS), jax.random.fold_in(arg_keys[0], 1), 0, BINS - 1).astype(jnp.int32),
        "leaf_ids": touch_ends(skewed_ids(arg_keys[1], (ROW_TOTAL,), LEAVES, 2), jax.random.fold_in(arg_keys[1], 3), 0, LEAVES - 1).astype(jnp.int32),
        "gradients": noise(arg_keys[2], (ROW_TOTAL,), 0.5, 3.0, ((0, 128),)),
        "hessians": jnp.clip(jnp.exp(math.log(0.25) - 1.6133518 * jax.random.uniform(arg_keys[3], (ROW_TOTAL,), jnp.float32) ** block_levels(arg_keys[3], (ROW_TOTAL,), ((0, 128),), -0.2, 0.2)), 0.049804688, 0.25).astype(jnp.bfloat16),
    }


reg_lambda = 1.0


def gain_of(left_grad, left_hess):
    total_grad = left_grad[:, :, -1:]
    total_hess = left_hess[:, :, -1:]
    right_grad = total_grad - left_grad
    right_hess = total_hess - left_hess
    return 0.5 * (left_grad * left_grad / (left_hess + reg_lambda)
                  + right_grad * right_grad / (right_hess + reg_lambda)
                  - total_grad * total_grad / (total_hess + reg_lambda))


def reference(bin_index, leaf_ids, gradients, hessians):
    grad_wide = gradients.astype(jnp.float32)
    hess_wide = hessians.astype(jnp.float32)
    group_width = math.gcd(FEATURES, 16)
    block_count = FEATURES // group_width
    segment_total = group_width * LEAVES * BINS

    def one_block(columns):
        offsets = jnp.arange(group_width, dtype=jnp.int32) * (LEAVES * BINS)
        flat_index = offsets[None, :] + leaf_ids[:, None] * BINS + columns
        flat_index = flat_index.reshape(-1)
        grad_flat = jnp.broadcast_to(grad_wide[:, None], columns.shape).reshape(-1)
        hess_flat = jnp.broadcast_to(hess_wide[:, None], columns.shape).reshape(-1)
        grad_hist = jax.ops.segment_sum(grad_flat, flat_index, num_segments=segment_total)
        hess_hist = jax.ops.segment_sum(hess_flat, flat_index, num_segments=segment_total)
        return (grad_hist.reshape(group_width, LEAVES, BINS), hess_hist.reshape(group_width, LEAVES, BINS))

    blocked = bin_index.reshape(ROW_TOTAL, block_count, group_width).transpose(1, 0, 2)
    hist_grad, hist_hess = lax.map(one_block, blocked)
    hist_grad = hist_grad.reshape(FEATURES, LEAVES, BINS)
    hist_hess = hist_hess.reshape(FEATURES, LEAVES, BINS)
    left_grad = jnp.cumsum(hist_grad, axis=2)
    left_hess = jnp.cumsum(hist_hess, axis=2)
    split_gains = gain_of(left_grad, left_hess)
    best_gain = jnp.max(split_gains, axis=(0, 2))
    return split_gains.reshape(N_FEAT, FEATURES // N_FEAT, LEAVES, BINS), best_gain
```

```python
import jax
import jax.numpy as jnp
from jax import lax
from jax.experimental import pallas as pl
from jax.experimental.pallas import tpu as pltpu
from jax.sharding import Mesh
from jax.sharding import PartitionSpec as P

f32, bf16 = jnp.float32, jnp.bfloat16
MESH = pl.DeviceIdType.MESH
BITS = ("z2", "z1", "z0", "y2", "y1", "y0", "xl", "xh", "co")
ROWS, FEAT = BITS[:7], BITS[7:]
CUBE = ("z0", "y0", "xl")
RING = ("z2", "z1", "y2", "y1")
ROUNDS = (("co", "xh", "xl"), ("y2", "y1", "y0"), ("z2", "z1", "z0"))
MSG = 304
reg_lambda = 1.0


def subset(axes, index):
    return tuple(a for i, a in enumerate(axes) if index >> (len(axes) - 1 - i) & 1)


def peer(flips):
    return {a: 1 - lax.axis_index(a) for a in flips}


def column(flips):
    j = 0
    for a in ROWS:
        b = lax.axis_index(a)
        j = 2 * j + (1 - b if a in flips else b)
    return j


def row(ref, slot, r):
    return jnp.broadcast_to(ref[slot, r:r + 1, :], (16, 128)).astype(bf16)


def side(ref, slot, fs, qs, n, vals, row16):
    zero = jnp.zeros((), bf16)
    cols = []
    for k, q in enumerate(qs):
        rows = []
        for f in fs:
            key = row(ref, slot, f * 16 + q)
            masks = [key == row16 + bf16(16 * i) for i in range(n // 16)]
            for v in vals[k]:
                rows += [jnp.where(m, v, zero) for m in masks]
        cols.append(jnp.concatenate(rows, axis=0))
    return jnp.concatenate(cols, axis=1)


def prep_slot(slot, rbuf, lof, hif, metaf):
    leaf = rbuf[slot, 256:272, :].astype(f32)
    metaf[slot] = rbuf[slot, 272:304, :].astype(f32)
    for f in range(16):
        b = rbuf[slot, f * 16:(f + 1) * 16, :].astype(f32)
        w = 64.0 if f % 8 < 4 else 32.0
        hi = jnp.floor(b * (1.0 / w))
        lof[slot, f * 16:(f + 1) * 16, :] = b - w * hi
        hif[slot, f * 16:(f + 1) * 16, :] = hi * 16.0 + leaf


def tiles(slot, base, lof, hif, metaf, accs):
    row16 = lax.broadcasted_iota(jnp.int32, (16, 128), 0).astype(f32).astype(bf16)
    one = jnp.ones((), bf16)
    stage = [0, 0]

    def tile(mxu, acc, fs, qs, vals, a, b):
        fs = [base + f for f in fs]
        rhs = side(lof, slot, fs, qs, b, vals, row16)
        lhs = side(hif, slot, fs, qs, a, [[one], [one]], row16)
        pltpu.matmul_push_rhs(rhs, stage[mxu], mxu, transpose=True)
        pltpu.matmul_acc_lhs(acc, lhs, stage[mxu])
        stage[mxu] ^= 1

    for qp in range(8):
        qs = (2 * qp, 2 * qp + 1)
        vals = [[row(metaf, slot, q), row(metaf, slot, 16 + q)] for q in qs]
        tile(qp % 2, accs[2 + qp % 2], (4, 5, 6, 7), qs, vals, 128, 32)
        for fp in range(2):
            tile(fp, accs[fp], (2 * fp, 2 * fp + 1), qs, vals, 64, 64)


def pop_hists(accs, hs, base):
    for fp in range(2):
        r = pltpu.matmul_pop(accs[fp])
        hs[base + 2 * fp] = r[:64, :128]
        hs[base + 2 * fp + 1] = r[64:, 128:]
    both = pltpu.matmul_pop(accs[2]) + pltpu.matmul_pop(accs[3])
    for f in range(4):
        r = both[f * 128:(f + 1) * 128, f * 64:(f + 1) * 64]
        parts = []
        for h in range(4):
            e, o = r[32 * h:32 * h + 16], r[32 * h + 16:32 * h + 32]
            parts.append(jnp.concatenate([e[:, :32], o[:, :32], e[:, 32:], o[:, 32:]], axis=1))
        hs[base + 4 + f] = jnp.concatenate(parts, axis=0)


def prefix_over_lo(h, acc):
    r = lax.broadcasted_iota(jnp.int32, (256, 256), 0) & 127
    c = lax.broadcasted_iota(jnp.int32, (256, 256), 1)
    ones = jnp.where(((r < 64) & (c < 64) & (r <= c)) | ((r >= 64) & (c >= 64) & (c < 128) & (r <= c)), 1.0, 0.0).astype(bf16)
    h1 = h.astype(bf16)
    rest = h - h1.astype(f32)
    h2 = rest.astype(bf16)
    h3 = (rest - h2.astype(f32)).astype(bf16)
    pltpu.matmul_push_rhs(ones, 0, 0)
    pltpu.matmul_acc_lhs(acc, jnp.concatenate([h1, h2], axis=1), 0)
    pltpu.matmul_acc_lhs(acc, jnp.concatenate([h3, jnp.zeros_like(h3)], axis=1), None)
    return pltpu.matmul_pop(acc)[:, :128]


def left_sums(p):
    outs = []
    for v in range(2):
        offset = jnp.zeros((16, 1), f32)
        parts = []
        for hi in range(4):
            block = p[hi * 16:(hi + 1) * 16, v * 64:(v + 1) * 64]
            parts.append(block + offset)
            offset = offset + block[:, 63:64]
        outs.append(jnp.concatenate(parts, axis=1))
    return outs


def gain_of(left_grad, left_hess):
    total_grad = left_grad[:, 255:256]
    total_hess = left_hess[:, 255:256]
    right_grad = total_grad - left_grad
    right_hess = total_hess - left_hess
    return 0.5 * (
        left_grad * left_grad / (left_hess + reg_lambda)
        + right_grad * right_grad / (right_hess + reg_lambda)
        - total_grad * total_grad / (total_hess + reg_lambda)
    )


def kernel(bins, leaf, grad, hess, gains, best, tbuf, sbuf, rbuf, lof, hif, metaf, hs, rs, mine, theirs,
           row_send, row_recv, part_send, part_recv, max_send, max_recv):
    partners = {subset(CUBE, c) for c in range(1, 8)} | {subset(RING, e) for e in range(1, 16)}
    partners |= {subset(axes, m) for axes in ROUNDS for m in range(1, 8)}
    partners = sorted({tuple(sorted(p)) for p in partners})
    barrier = pltpu.get_barrier_semaphore()
    for p in partners:
        pl.semaphore_signal(barrier, inc=1, device_id=peer(p), device_id_type=MESH)

    for q in range(16):
        tbuf[pl.ds(q, 128, stride=16), :] = bins[q * 128:(q + 1) * 128, :].astype(f32).T
    meta = [leaf[...].astype(f32).astype(bf16), grad[...], hess[...]]

    def pack(c, store):
        for e in range(16):
            j = column(subset(CUBE, c) + subset(RING, e))
            store(e * 16, tbuf[pl.ds(pl.multiple_of(j * 16, 16), 16), :].astype(bf16))
        for i, m in enumerate(meta):
            store(256 + 16 * i, m)

    def to_sbuf(c):
        def store(r, v):
            sbuf[c, r:r + 16, :] = v
        return store

    def to_own(r, v):
        rbuf[0, r:r + 16, :] = v

    for c in range(7, 0, -1):
        pack(c, to_sbuf(c))

    def row_copy(c):
        return pltpu.make_async_remote_copy(
            src_ref=sbuf.at[c], dst_ref=rbuf.at[c], send_sem=row_send.at[c], recv_sem=row_recv.at[c],
            device_id=peer(subset(CUBE, c)), device_id_type=MESH)

    pl.semaphore_wait(barrier, len(partners))
    for c in range(7, 0, -1):
        row_copy(c).start()
    pack(0, to_own)

    def part_copy(e):
        return pltpu.make_async_remote_copy(
            src_ref=hs.at[e], dst_ref=rs.at[e], send_sem=part_send.at[e], recv_sem=part_recv.at[e],
            device_id=peer(subset(RING, e)), device_id_type=MESH)

    def scoped(*accs):
        prep_slot(0, rbuf, lof, hif, metaf)
        tiles(0, 8, lof, hif, metaf, accs)

        @pl.loop(1, 8)
        def _(s):
            pltpu.make_async_remote_copy(
                src_ref=sbuf.at[s], dst_ref=rbuf.at[s], send_sem=row_send.at[s], recv_sem=row_recv.at[s],
                device_id=peer(CUBE), device_id_type=MESH).wait_recv()
            prep_slot(s, rbuf, lof, hif, metaf)
            tiles(s, 8, lof, hif, metaf, accs)

        pop_hists(accs, hs, 8)
        for e in range(15, 7, -1):
            part_copy(e).start()

        @pl.loop(0, 8)
        def _(s):
            tiles(s, 0, lof, hif, metaf, accs)

        pop_hists(accs, hs, 0)
        for e in range(7, 0, -1):
            part_copy(e).start()

        total = hs[0]
        for e in range(15, 0, -1):
            part_copy(e).wait_recv()
            total = total + rs[e]
        left_grad, left_hess = left_sums(prefix_over_lo(total, accs[4]))
        gain = gain_of(left_grad, left_hess)
        gains[...] = gain
        top = jnp.broadcast_to(jnp.max(gain, axis=1, keepdims=True), (16, 128))
        sub = lax.broadcasted_iota(jnp.int32, (16, 128), 0)
        lane = lax.broadcasted_iota(jnp.int32, (16, 128), 1)
        here = jnp.max(jnp.where(sub == lane, top, -jnp.inf), axis=0, keepdims=True)
        for k, axes in enumerate(ROUNDS):
            mine[k] = here
            copies = [pltpu.make_async_remote_copy(
                src_ref=mine.at[k], dst_ref=theirs.at[8 * k + m], send_sem=max_send.at[8 * k + m], recv_sem=max_recv.at[8 * k + m],
                device_id=peer(subset(axes, m)), device_id_type=MESH) for m in range(1, 8)]
            for copy in copies:
                copy.start()
            for m, copy in enumerate(copies):
                copy.wait_recv()
                here = jnp.maximum(here, theirs[8 * k + m + 1])
            for copy in copies:
                copy.wait_send()
        best[...] = here

    pl.run_scoped(
        scoped, pltpu.ACC(0)((128, 256), f32), pltpu.ACC(1)((128, 256), f32), pltpu.ACC(0)((512, 256), f32),
        pltpu.ACC(1)((512, 256), f32), pltpu.ACC(0)((64, 256), f32))
    for c in range(1, 8):
        row_copy(c).wait_send()
    for e in range(1, 16):
        part_copy(e).wait_send()


def body(bin_index, leaf_ids, gradients, hessians):
    vmem = pl.BlockSpec(memory_space=pltpu.VMEM)
    gains, best = pl.pallas_call(
        kernel,
        out_shape=(jax.ShapeDtypeStruct((16, 256), f32), jax.ShapeDtypeStruct((1, 128), f32)),
        in_specs=[vmem] * 4,
        out_specs=(vmem, vmem),
        scratch_shapes=[
            pltpu.VMEM((2048, 128), f32),
            pltpu.VMEM((8, MSG, 128), bf16),
            pltpu.VMEM((8, MSG, 128), bf16),
            pltpu.VMEM((8, 256, 128), f32),
            pltpu.VMEM((8, 256, 128), f32),
            pltpu.VMEM((8, 32, 128), f32),
            pltpu.VMEM((16, 64, 128), f32),
            pltpu.VMEM((16, 64, 128), f32),
            pltpu.VMEM((3, 1, 128), f32),
            pltpu.VMEM((24, 1, 128), f32),
            pltpu.SemaphoreType.DMA((8,)),
            pltpu.SemaphoreType.DMA((8,)),
            pltpu.SemaphoreType.DMA((16,)),
            pltpu.SemaphoreType.DMA((16,)),
            pltpu.SemaphoreType.DMA((24,)),
            pltpu.SemaphoreType.DMA((24,)),
        ],
        compiler_params=pltpu.CompilerParams(collective_id=0, has_side_effects=True, vmem_limit_bytes=48 * 1024 * 1024),
    )(bin_index, leaf_ids.reshape(16, 128), gradients.reshape(16, 128), hessians.reshape(16, 128))
    return gains[None, None], best[0, :LEAVES]


LEAVES = 16


def solution(mesh):
    bits = Mesh(mesh.devices.reshape((2,) * 9), BITS)
    return jax.shard_map(
        body,
        mesh=bits,
        in_specs=(P(ROWS, FEAT), P(ROWS), P(ROWS), P(ROWS)),
        out_specs=(P(FEAT, ROWS, None, None), P()),
        check_vma=False,
    )
```

```python
import jax
import jax.numpy as jnp
from jax import lax
from jax.experimental import pallas as pl
from jax.experimental.pallas import tpu as pltpu
from jax.sharding import Mesh
from jax.sharding import PartitionSpec as P

f32, bf16 = jnp.float32, jnp.bfloat16
MESH = pl.DeviceIdType.MESH
BITS = ("z2", "z1", "z0", "y2", "y1", "y0", "xl", "xh", "co")
ROWS, FEAT = BITS[:7], BITS[7:]
CUBE = ("z0", "y0", "xl")
RING = ("z2", "z1", "y2", "y1")
CUBES = [(), ("xl",), ("y0",), ("z0",), ("y0", "xl"), ("z0", "xl"), ("z0", "y0"), ("z0", "y0", "xl")]
PASSES = ((10, 15, 14, 11, 8, 2, 9, 6), (7, 13, 5, 12, 3, 4, 1, 0))
LINES = (("co", "xh", "xl"), ("y2", "y1", "y0"), ("z2", "z1", "z0"))
ROUNDS = (("z2", "z1", "z0", "co"), ("y2", "y1", "y0", "xh", "xl"))
FIRST = (0, 15)
META = 128
MSG = (176, 128)
reg_lambda = 1.0


def subset(axes, index):
    return tuple(a for i, a in enumerate(axes) if index >> (len(axes) - 1 - i) & 1)


def peer(flips):
    return {a: 1 - lax.axis_index(a) for a in flips}


def column(flips):
    j = 0
    for a in ROWS:
        b = lax.axis_index(a)
        j = 2 * j + (1 - b if a in flips else b)
    return j


def row(ref, slot, r):
    return jnp.broadcast_to(ref[slot, r:r + 1, :], (16, 128)).astype(bf16)


def side(ref, slot, fs, qs, n, vals, row16):
    zero = jnp.zeros((), bf16)
    cols = []
    for k, q in enumerate(qs):
        rows = []
        for f in fs:
            key = row(ref, slot, f * 16 + q)
            masks = [key == row16 + bf16(16 * i) for i in range(n // 16)]
            for v in vals[k]:
                rows += [jnp.where(m, v, zero) for m in masks]
        cols.append(jnp.concatenate(rows, axis=0))
    return jnp.concatenate(cols, axis=1)


def prep_meta(slot, rbuf, leaff, metaf):
    leaff[slot] = rbuf[slot, META:META + 16, :].astype(f32)
    metaf[slot] = rbuf[slot, META + 16:META + 48, :].astype(f32)


def prep_slot(g, slot, rbuf, lof, hif, leaff):
    leaf = leaff[slot]
    for f in range(8):
        b = rbuf[slot, f * 16:(f + 1) * 16, :].astype(f32)
        w = 64.0 if f < 4 else 32.0
        hi = jnp.floor(b * (1.0 / w))
        lof[slot, f * 16:(f + 1) * 16, :] = b - w * hi
        hif[slot, f * 16:(f + 1) * 16, :] = hi * 16.0 + leaf


def tiles(slot, lof, hif, metaf, accs):
    row16 = lax.broadcasted_iota(jnp.int32, (16, 128), 0).astype(f32).astype(bf16)
    one = jnp.ones((), bf16)
    stage = [0, 0]

    def tile(mxu, acc, fs, qs, vals, a, b):
        rhs = side(lof, slot, fs, qs, b, vals, row16)
        lhs = side(hif, slot, fs, qs, a, [[one], [one]], row16)
        pltpu.matmul_push_rhs(rhs, stage[mxu], mxu, transpose=True)
        pltpu.matmul_acc_lhs(acc, lhs, stage[mxu])
        stage[mxu] ^= 1

    for qp in range(8):
        qs = (2 * qp, 2 * qp + 1)
        vals = [[row(metaf, slot, q), row(metaf, slot, 16 + q)] for q in qs]
        tile(qp % 2, accs[2 + qp % 2], (4, 5, 6, 7), qs, vals, 128, 32)
        for fp in range(2):
            tile(fp, accs[fp], (2 * fp, 2 * fp + 1), qs, vals, 64, 64)


def pop_hists(accs, hs, es, more=False):
    def put(e, v):
        hs[e] = hs[e] + v if more else v

    for fp in range(2):
        r = pltpu.matmul_pop(accs[fp])
        put(es[2 * fp], r[:64, :128])
        put(es[2 * fp + 1], r[64:, 128:])
    both = pltpu.matmul_pop(accs[2]) + pltpu.matmul_pop(accs[3])
    for f in range(4):
        r = both[f * 128:(f + 1) * 128, f * 64:(f + 1) * 64]
        parts = []
        for h in range(4):
            e, o = r[32 * h:32 * h + 16], r[32 * h + 16:32 * h + 32]
            parts.append(jnp.concatenate([e[:, :32], o[:, :32], e[:, 32:], o[:, 32:]], axis=1))
        put(es[4 + f], jnp.concatenate(parts, axis=0))


def prefix_over_lo(h, acc):
    r = lax.broadcasted_iota(jnp.int32, (256, 256), 0) & 127
    c = lax.broadcasted_iota(jnp.int32, (256, 256), 1)
    ones = jnp.where(((r < 64) & (c < 64) & (r <= c)) | ((r >= 64) & (c >= 64) & (c < 128) & (r <= c)), 1.0, 0.0).astype(bf16)
    h1 = h.astype(bf16)
    rest = h - h1.astype(f32)
    h2 = rest.astype(bf16)
    h3 = (rest - h2.astype(f32)).astype(bf16)
    pltpu.matmul_push_rhs(ones, 0, 0)
    pltpu.matmul_acc_lhs(acc, jnp.concatenate([h1, h2], axis=1), 0)
    pltpu.matmul_acc_lhs(acc, jnp.concatenate([h3, jnp.zeros_like(h3)], axis=1), None)
    return pltpu.matmul_pop(acc)[:, :128]


def left_sums(p):
    outs = []
    for v in range(2):
        offset = jnp.zeros((16, 1), f32)
        parts = []
        for hi in range(4):
            block = p[hi * 16:(hi + 1) * 16, v * 64:(v + 1) * 64]
            parts.append(block + offset)
            offset = offset + block[:, 63:64]
        outs.append(jnp.concatenate(parts, axis=1))
    return outs


def gain_of(left_grad, left_hess):
    total_grad = left_grad[:, 255:256]
    total_hess = left_hess[:, 255:256]
    right_grad = total_grad - left_grad
    right_hess = total_hess - left_hess
    return 0.5 * (
        left_grad * left_grad / (left_hess + reg_lambda)
        + right_grad * right_grad / (right_hess + reg_lambda)
        - total_grad * total_grad / (total_hess + reg_lambda)
    )


def kernel(bins_hbm, leaf_hbm, grad_hbm, hess_hbm, gains, best, bins, leaf, grad, hess, tbuf, sbuf0, sbuf1, rbuf0, rbuf1,
           lof, hif, leaff, metaf, hs, rs, mine, theirs,
           in_sem, row_send, row_recv, part_send, part_recv, max_send, max_recv, relay_sem):
    loads = [pltpu.make_async_copy(bins_hbm.at[pl.ds(i * 1024, 1024)], bins.at[pl.ds(i * 1024, 1024)], in_sem.at[i]) for i in range(2)]
    loads += [pltpu.make_async_copy(a, b, in_sem.at[2 + i])
              for i, (a, b) in enumerate(((leaf_hbm, leaf), (grad_hbm, grad), (hess_hbm, hess)))]
    for load in loads:
        load.start()
    partners = set(CUBES[1:]) | {subset(axes, m) for axes in LINES for m in range(1, 8)}
    partners = sorted({tuple(sorted(p)) for p in partners})
    relays = [subset(("y2", "y1"), m) for m in range(1, 4)] + [("co",)] + [subset(("xh", "xl"), m) for m in range(1, 4)]
    barrier = pltpu.get_barrier_semaphore()
    for p in partners:
        pl.semaphore_signal(barrier, inc=1, device_id=peer(p), device_id_type=MESH)

    for q in range(16):
        if q % 8 == 0:
            loads[q // 8].wait()
        tbuf[pl.ds(q, 128, stride=16), :] = bins[q * 128:(q + 1) * 128, :].astype(f32).T
    for load in loads[2:]:
        load.wait()
    meta = [leaf[...].astype(f32).astype(bf16), grad[...], hess[...]]
    sbufs, rbufs = (sbuf0, sbuf1), (rbuf0, rbuf1)

    def pack(g, c):
        buf = sbufs[g] if c else rbufs[g]
        for i, e in enumerate(PASSES[g]):
            j = column(CUBES[c] + subset(RING, e))
            buf[c, i * 16:(i + 1) * 16, :] = tbuf[pl.ds(pl.multiple_of(j * 16, 16), 16), :].astype(bf16)
        if g == 0:
            for i, m in enumerate(meta):
                buf[c, META + 16 * i:META + 16 * (i + 1), :] = m

    def row_copy(g, c, flips):
        return pltpu.make_async_remote_copy(
            src_ref=sbufs[g].at[c], dst_ref=rbufs[g].at[c], send_sem=row_send.at[8 * g + c], recv_sem=row_recv.at[8 * g + c],
            device_id=peer(flips), device_id_type=MESH)

    for c in range(1, 8):
        pack(0, c)
    for g in (1, 0):
        pack(g, 0)
    def part_copy(e):
        return pltpu.make_async_remote_copy(
            src_ref=hs.at[e], dst_ref=rs.at[e], send_sem=part_send.at[e], recv_sem=part_recv.at[e],
            device_id=peer(subset(RING, e)), device_id_type=MESH)

    def scoped(*accs):
        prep_meta(0, rbuf0, leaff, metaf)
        prep_slot(1, 0, rbuf1, lof, hif, leaff)
        tiles(0, lof, hif, metaf, accs)
        pop_hists(accs, hs, PASSES[1])
        for c in range(1, 8):
            pack(1, c)
        pl.semaphore_wait(barrier, len(partners))
        for c in range(1, 8):
            row_copy(0, c, CUBES[c]).start()
        for p in relays:
            pl.semaphore_signal(relay_sem, inc=1, device_id=peer(p), device_id_type=MESH)
        prep_slot(0, 0, rbuf0, lof, hif, leaff)
        tiles(0, lof, hif, metaf, accs)

        def rest(g, lo, hi):
            @pl.loop(lo, hi)
            def _(s):
                row_copy(g, s, CUBE).wait_recv()
                if g == 0:
                    prep_meta(s, rbuf0, leaff, metaf)
                prep_slot(g, s, rbufs[g], lof, hif, leaff)
                tiles(s, lof, hif, metaf, accs)

        rest(0, 1, 4)
        for c in range(1, 8):
            row_copy(1, c, CUBES[c]).start()
        rest(0, 4, 8)
        for g in range(2):
            if g:
                rest(1, 1, 8)
            pop_hists(accs, hs, PASSES[g], more=g == 1)
            if g == 0:
                pl.semaphore_wait(relay_sem, len(relays))
            for e in PASSES[g]:
                if e:
                    part_copy(e).start()

        total = hs[0]
        for e in PASSES[0] + PASSES[1][:7]:
            part_copy(e).wait_recv()
            total = total + rs[e]
        left_grad, left_hess = left_sums(prefix_over_lo(total, accs[4]))
        gain = gain_of(left_grad, left_hess)
        gains[...] = gain
        top = jnp.broadcast_to(jnp.max(gain, axis=1, keepdims=True), (16, 128))
        sub = lax.broadcasted_iota(jnp.int32, (16, 128), 0)
        lane = lax.broadcasted_iota(jnp.int32, (16, 128), 1)
        here = jnp.max(jnp.where(sub == lane, top, -jnp.inf), axis=0, keepdims=True)
        sent = []
        for k, axes in enumerate(ROUNDS):
            mine[k] = here
            steps = range(1, 1 << len(axes))
            copies = [pltpu.make_async_remote_copy(
                src_ref=mine.at[k], dst_ref=theirs.at[FIRST[k] + m - 1], send_sem=max_send.at[FIRST[k] + m - 1],
                recv_sem=max_recv.at[FIRST[k] + m - 1], device_id=peer(subset(axes, m)), device_id_type=MESH) for m in steps]
            for copy in reversed(copies):
                copy.start()
            for copy in copies:
                copy.wait_recv()
            here = jnp.maximum(here, jnp.max(theirs[FIRST[k]:FIRST[k] + len(steps)], axis=0))
            sent += copies
        best[...] = here
        for copy in sent:
            copy.wait_send()

    pl.run_scoped(
        scoped, pltpu.ACC(0)((128, 256), f32), pltpu.ACC(1)((128, 256), f32), pltpu.ACC(0)((512, 256), f32),
        pltpu.ACC(1)((512, 256), f32), pltpu.ACC(0)((64, 256), f32))
    for g in range(2):
        for c in range(1, 8):
            row_copy(g, c, CUBES[c]).wait_send()
    for e in range(1, 16):
        part_copy(e).wait_send()


def body(bin_index, leaf_ids, gradients, hessians):
    vmem = pl.BlockSpec(memory_space=pltpu.VMEM)
    gains, best = pl.pallas_call(
        kernel,
        out_shape=(jax.ShapeDtypeStruct((16, 256), f32), jax.ShapeDtypeStruct((1, 128), f32)),
        in_specs=[pl.BlockSpec(memory_space=pltpu.HBM)] * 4,
        out_specs=(vmem, vmem),
        scratch_shapes=[
            pltpu.VMEM((2048, 128), jnp.int32),
            pltpu.VMEM((16, 128), jnp.int32),
            pltpu.VMEM((16, 128), bf16),
            pltpu.VMEM((16, 128), bf16),
            pltpu.VMEM((2048, 128), f32),
            pltpu.VMEM((8, MSG[0], 128), bf16),
            pltpu.VMEM((8, MSG[1], 128), bf16),
            pltpu.VMEM((8, MSG[0], 128), bf16),
            pltpu.VMEM((8, MSG[1], 128), bf16),
            pltpu.VMEM((8, 128, 128), f32),
            pltpu.VMEM((8, 128, 128), f32),
            pltpu.VMEM((8, 16, 128), f32),
            pltpu.VMEM((8, 32, 128), f32),
            pltpu.VMEM((16, 64, 128), f32),
            pltpu.VMEM((16, 64, 128), f32),
            pltpu.VMEM((2, 1, 128), f32),
            pltpu.VMEM((46, 1, 128), f32),
            pltpu.SemaphoreType.DMA((5,)),
            pltpu.SemaphoreType.DMA((16,)),
            pltpu.SemaphoreType.DMA((16,)),
            pltpu.SemaphoreType.DMA((16,)),
            pltpu.SemaphoreType.DMA((16,)),
            pltpu.SemaphoreType.DMA((46,)),
            pltpu.SemaphoreType.DMA((46,)),
            pltpu.SemaphoreType.REGULAR,
        ],
        compiler_params=pltpu.CompilerParams(collective_id=0, has_side_effects=True, vmem_limit_bytes=48 * 1024 * 1024),
    )(*(pltpu.with_memory_space_constraint(a, pltpu.HBM) for a in (
        bin_index, leaf_ids.reshape(16, 128), gradients.reshape(16, 128), hessians.reshape(16, 128))))
    return gains[None, None], best[0, :LEAVES]


LEAVES = 16


def solution(mesh):
    bits = Mesh(mesh.devices.reshape((2,) * 9), BITS)
    return jax.shard_map(
        body,
        mesh=bits,
        in_specs=(P(ROWS, FEAT), P(ROWS), P(ROWS), P(ROWS)),
        out_specs=(P(FEAT, ROWS, None, None), P()),
        check_vma=False,
    )
```

```python
import jax
import jax.numpy as jnp
from jax import lax
from jax.experimental import pallas as pl
from jax.experimental.pallas import tpu as pltpu
from jax.sharding import Mesh
from jax.sharding import PartitionSpec as P

f32, bf16 = jnp.float32, jnp.bfloat16
MESH = pl.DeviceIdType.MESH
BITS = ("z2", "z1", "z0", "y2", "y1", "y0", "xl", "xh", "co")
ROWS, FEAT = BITS[:7], BITS[7:]
CUBE = ("z0", "y0", "xl")
CUBES = [(), ("xl",), ("y0",), ("z0",), ("y0", "xl"), ("z0", "xl"), ("z0", "y0"), ("z0", "y0", "xl")]
PASSES = ((10, 15, 14, 11, 8, 2, 9, 6), (7, 13, 5, 12, 3, 4, 1, 0))
LINES = (("co", "xh", "xl"), ("y2", "y1", "y0"), ("z2", "z1", "z0"))
ROUNDS = (("z2", "z1", "z0", "co"), ("y2", "y1", "y0", "xh", "xl"))
FIRST = (0, 15)
META = 128
MSG = (176, 128)
reg_lambda = 1.0


def ring(e):
    z, y = (((), ("z1",), ("z2", "z0"), ("z2", "z1"))[e // 4], ((), ("y1",), ("y2", "y0"), ("y2", "y1"))[e % 4])
    return z + y


def subset(axes, index):
    return tuple(a for i, a in enumerate(axes) if index >> (len(axes) - 1 - i) & 1)


def peer(flips):
    return {a: 1 - lax.axis_index(a) for a in flips}


def column(flips):
    j = 0
    for a in ROWS:
        b = lax.axis_index(a)
        j = 2 * j + (1 - b if a in flips else b)
    return j


def row(ref, slot, r):
    return jnp.broadcast_to(ref[slot, r:r + 1, :], (16, 128)).astype(bf16)


def side(ref, slot, fs, qs, n, vals, row16):
    zero = jnp.zeros((), bf16)
    cols = []
    for k, q in enumerate(qs):
        rows = []
        for f in fs:
            key = row(ref, slot, f * 16 + q)
            masks = [key == row16 + bf16(16 * i) for i in range(n // 16)]
            for v in vals[k]:
                rows += [jnp.where(m, v, zero) for m in masks]
        cols.append(jnp.concatenate(rows, axis=0))
    return jnp.concatenate(cols, axis=1)


def prep_meta(slot, rbuf, leaff, metaf):
    leaff[slot] = rbuf[slot, META:META + 16, :].astype(f32)
    metaf[slot] = rbuf[slot, META + 16:META + 48, :].astype(f32)


def prep_slot(g, slot, rbuf, lof, hif, leaff):
    leaf = leaff[slot]
    for f in range(8):
        b = rbuf[slot, f * 16:(f + 1) * 16, :].astype(f32)
        w = 64.0 if f < 4 else 32.0
        hi = jnp.floor(b * (1.0 / w))
        lof[slot, f * 16:(f + 1) * 16, :] = b - w * hi
        hif[slot, f * 16:(f + 1) * 16, :] = hi * 16.0 + leaf


def tiles(slot, lof, hif, metaf, accs):
    row16 = lax.broadcasted_iota(jnp.int32, (16, 128), 0).astype(f32).astype(bf16)
    one = jnp.ones((), bf16)
    stage = [0, 0]

    def tile(mxu, acc, fs, qs, vals, a, b):
        rhs = side(lof, slot, fs, qs, b, vals, row16)
        lhs = side(hif, slot, fs, qs, a, [[one], [one]], row16)
        pltpu.matmul_push_rhs(rhs, stage[mxu], mxu, transpose=True)
        pltpu.matmul_acc_lhs(acc, lhs, stage[mxu])
        stage[mxu] ^= 1

    for qp in range(8):
        qs = (2 * qp, 2 * qp + 1)
        vals = [[row(metaf, slot, q), row(metaf, slot, 16 + q)] for q in qs]
        tile(qp % 2, accs[2 + qp % 2], (4, 5, 6, 7), qs, vals, 128, 32)
        for fp in range(2):
            tile(fp, accs[fp], (2 * fp, 2 * fp + 1), qs, vals, 64, 64)


def pop_hists(accs, hs, es, more=False):
    def put(e, v):
        hs[e] = hs[e] + v if more else v

    for fp in range(2):
        r = pltpu.matmul_pop(accs[fp])
        put(es[2 * fp], r[:64, :128])
        put(es[2 * fp + 1], r[64:, 128:])
    both = pltpu.matmul_pop(accs[2]) + pltpu.matmul_pop(accs[3])
    for f in range(4):
        r = both[f * 128:(f + 1) * 128, f * 64:(f + 1) * 64]
        parts = []
        for h in range(4):
            e, o = r[32 * h:32 * h + 16], r[32 * h + 16:32 * h + 32]
            parts.append(jnp.concatenate([e[:, :32], o[:, :32], e[:, 32:], o[:, 32:]], axis=1))
        put(es[4 + f], jnp.concatenate(parts, axis=0))


def prefix_over_lo(h, acc):
    r = lax.broadcasted_iota(jnp.int32, (256, 256), 0) & 127
    c = lax.broadcasted_iota(jnp.int32, (256, 256), 1)
    ones = jnp.where(((r < 64) & (c < 64) & (r <= c)) | ((r >= 64) & (c >= 64) & (c < 128) & (r <= c)), 1.0, 0.0).astype(bf16)
    pltpu.matmul_push_rhs(ones, 0, 0)
    h1 = h.astype(bf16)
    rest = h - h1.astype(f32)
    h2 = rest.astype(bf16)
    h3 = (rest - h2.astype(f32)).astype(bf16)
    pltpu.matmul_acc_lhs(acc, jnp.concatenate([h1, h2], axis=1), 0)
    pltpu.matmul_acc_lhs(acc, jnp.concatenate([h3, jnp.zeros_like(h3)], axis=1), None)
    return pltpu.matmul_pop(acc)[:, :128]


def left_sums(p):
    outs = []
    for v in range(2):
        offset = jnp.zeros((16, 1), f32)
        parts = []
        for hi in range(4):
            block = p[hi * 16:(hi + 1) * 16, v * 64:(v + 1) * 64]
            parts.append(block + offset)
            offset = offset + block[:, 63:64]
        outs.append(jnp.concatenate(parts, axis=1))
    return outs


def gain_of(left_grad, left_hess):
    total_grad = left_grad[:, 255:256]
    total_hess = left_hess[:, 255:256]
    right_grad = total_grad - left_grad
    right_hess = total_hess - left_hess
    return 0.5 * (
        left_grad * left_grad / (left_hess + reg_lambda)
        + right_grad * right_grad / (right_hess + reg_lambda)
        - total_grad * total_grad / (total_hess + reg_lambda)
    )


def kernel(bins_hbm, leaf_hbm, grad_hbm, hess_hbm, gains, best, bins, leaf, grad, hess, tbuf, sbuf0, sbuf1, rbuf0, rbuf1,
           lof, hif, leaff, metaf, hs, rs, mine, theirs,
           in_sem, row_send, row_recv, part_send, part_recv, max_send, max_recv, relay_sem):
    loads = [pltpu.make_async_copy(bins_hbm.at[pl.ds(i * 1024, 1024)], bins.at[pl.ds(i * 1024, 1024)], in_sem.at[i]) for i in range(2)]
    loads += [pltpu.make_async_copy(a, b, in_sem.at[2 + i])
              for i, (a, b) in enumerate(((leaf_hbm, leaf), (grad_hbm, grad), (hess_hbm, hess)))]
    for load in loads:
        load.start()
    partners = set(CUBES[1:]) | {subset(axes, m) for axes in LINES for m in range(1, 8)}
    partners = sorted({tuple(sorted(p)) for p in partners})
    relays = [ring(e) for e in range(1, 4)] + [("co",)] + [subset(("xh", "xl"), m) for m in range(1, 4)]
    barrier = pltpu.get_barrier_semaphore()
    for p in partners:
        pl.semaphore_signal(barrier, inc=1, device_id=peer(p), device_id_type=MESH)

    for q in range(16):
        if q % 8 == 0:
            loads[q // 8].wait()
        tbuf[pl.ds(q, 128, stride=16), :] = bins[q * 128:(q + 1) * 128, :].astype(f32).T
    for load in loads[2:]:
        load.wait()
    meta = [leaf[...].astype(f32).astype(bf16), grad[...], hess[...]]
    sbufs, rbufs = (sbuf0, sbuf1), (rbuf0, rbuf1)

    def pack(g, c):
        buf = sbufs[g] if c else rbufs[g]
        for i, e in enumerate(PASSES[g]):
            j = column(set(CUBES[c]) ^ set(ring(e)))
            buf[c, i * 16:(i + 1) * 16, :] = tbuf[pl.ds(pl.multiple_of(j * 16, 16), 16), :].astype(bf16)
        if g == 0:
            for i, m in enumerate(meta):
                buf[c, META + 16 * i:META + 16 * (i + 1), :] = m

    def row_copy(g, c, flips):
        return pltpu.make_async_remote_copy(
            src_ref=sbufs[g].at[c], dst_ref=rbufs[g].at[c], send_sem=row_send.at[8 * g + c], recv_sem=row_recv.at[8 * g + c],
            device_id=peer(flips), device_id_type=MESH)

    for c in range(1, 8):
        pack(0, c)
    for g in (1, 0):
        pack(g, 0)
    def part_copy(e):
        return pltpu.make_async_remote_copy(
            src_ref=hs.at[e], dst_ref=rs.at[e], send_sem=part_send.at[e], recv_sem=part_recv.at[e],
            device_id=peer(ring(e)), device_id_type=MESH)

    def scoped(*accs):
        prep_meta(0, rbuf0, leaff, metaf)
        pl.semaphore_wait(barrier, len(partners))
        for c in range(1, 8):
            row_copy(0, c, CUBES[c]).start()
        for p in relays:
            pl.semaphore_signal(relay_sem, inc=1, device_id=peer(p), device_id_type=MESH)
        prep_slot(1, 0, rbuf1, lof, hif, leaff)
        tiles(0, lof, hif, metaf, accs)
        pop_hists(accs, hs, PASSES[1])
        for c in range(1, 8):
            pack(1, c)
        prep_slot(0, 0, rbuf0, lof, hif, leaff)
        tiles(0, lof, hif, metaf, accs)

        def rest(g, slots):
            for c in slots:
                row_copy(g, c, CUBES[c]).wait_recv()
            for c in slots:
                if g == 0:
                    prep_meta(c, rbuf0, leaff, metaf)
                prep_slot(g, c, rbufs[g], lof, hif, leaff)
            for c in slots:
                tiles(c, lof, hif, metaf, accs)

        for c in range(1, 8):
            row_copy(1, c, CUBES[c]).start()
        rest(0, range(1, 4))
        rest(0, range(4, 8))
        for g in range(2):
            if g:
                rest(1, range(1, 4))
                rest(1, range(4, 8))
            pop_hists(accs, hs, PASSES[g], more=g == 1)
            if g == 0:
                pl.semaphore_wait(relay_sem, len(relays))
            for e in PASSES[g]:
                if e:
                    part_copy(e).start()

        total = hs[0]
        for e in PASSES[0] + PASSES[1][:7]:
            part_copy(e).wait_recv()
            total = total + rs[e]
        left_grad, left_hess = left_sums(prefix_over_lo(total, accs[4]))
        gain = gain_of(left_grad, left_hess)
        gains[...] = gain
        top = jnp.broadcast_to(jnp.max(gain, axis=1, keepdims=True), (16, 128))
        sub = lax.broadcasted_iota(jnp.int32, (16, 128), 0)
        lane = lax.broadcasted_iota(jnp.int32, (16, 128), 1)
        here = jnp.max(jnp.where(sub == lane, top, -jnp.inf), axis=0, keepdims=True)
        sent = []
        for k, axes in enumerate(ROUNDS):
            mine[k] = here
            steps = range(1, 1 << len(axes))
            copies = [pltpu.make_async_remote_copy(
                src_ref=mine.at[k], dst_ref=theirs.at[FIRST[k] + m - 1], send_sem=max_send.at[FIRST[k] + m - 1],
                recv_sem=max_recv.at[FIRST[k] + m - 1], device_id=peer(subset(axes, m)), device_id_type=MESH) for m in steps]
            for copy in reversed(copies):
                copy.start()
            for copy in copies:
                copy.wait_recv()
            here = jnp.maximum(here, jnp.max(theirs[FIRST[k]:FIRST[k] + len(steps)], axis=0))
            sent += copies
        best[...] = here
        for copy in sent:
            copy.wait_send()

    pl.run_scoped(
        scoped, pltpu.ACC(0)((128, 256), f32), pltpu.ACC(1)((128, 256), f32), pltpu.ACC(0)((512, 256), f32),
        pltpu.ACC(1)((512, 256), f32), pltpu.ACC(0)((64, 256), f32))
    for g in range(2):
        for c in range(1, 8):
            row_copy(g, c, CUBES[c]).wait_send()
    for e in range(1, 16):
        part_copy(e).wait_send()


def body(bin_index, leaf_ids, gradients, hessians):
    vmem = pl.BlockSpec(memory_space=pltpu.VMEM)
    gains, best = pl.pallas_call(
        kernel,
        out_shape=(jax.ShapeDtypeStruct((16, 256), f32), jax.ShapeDtypeStruct((1, 128), f32)),
        in_specs=[pl.BlockSpec(memory_space=pltpu.HBM)] * 4,
        out_specs=(vmem, vmem),
        scratch_shapes=[
            pltpu.VMEM((2048, 128), jnp.int32),
            pltpu.VMEM((16, 128), jnp.int32),
            pltpu.VMEM((16, 128), bf16),
            pltpu.VMEM((16, 128), bf16),
            pltpu.VMEM((2048, 128), f32),
            pltpu.VMEM((8, MSG[0], 128), bf16),
            pltpu.VMEM((8, MSG[1], 128), bf16),
            pltpu.VMEM((8, MSG[0], 128), bf16),
            pltpu.VMEM((8, MSG[1], 128), bf16),
            pltpu.VMEM((8, 128, 128), f32),
            pltpu.VMEM((8, 128, 128), f32),
            pltpu.VMEM((8, 16, 128), f32),
            pltpu.VMEM((8, 32, 128), f32),
            pltpu.VMEM((16, 64, 128), f32),
            pltpu.VMEM((16, 64, 128), f32),
            pltpu.VMEM((2, 1, 128), f32),
            pltpu.VMEM((46, 1, 128), f32),
            pltpu.SemaphoreType.DMA((5,)),
            pltpu.SemaphoreType.DMA((16,)),
            pltpu.SemaphoreType.DMA((16,)),
            pltpu.SemaphoreType.DMA((16,)),
            pltpu.SemaphoreType.DMA((16,)),
            pltpu.SemaphoreType.DMA((46,)),
            pltpu.SemaphoreType.DMA((46,)),
            pltpu.SemaphoreType.REGULAR,
        ],
        compiler_params=pltpu.CompilerParams(collective_id=0, has_side_effects=True, vmem_limit_bytes=48 * 1024 * 1024),
    )(*(pltpu.with_memory_space_constraint(a, pltpu.HBM) for a in (
        bin_index, leaf_ids.reshape(16, 128), gradients.reshape(16, 128), hessians.reshape(16, 128))))
    return gains[None, None], best[0, :LEAVES]


LEAVES = 16


def solution(mesh):
    bits = Mesh(mesh.devices.reshape((2,) * 9), BITS)
    return jax.shard_map(
        body,
        mesh=bits,
        in_specs=(P(ROWS, FEAT), P(ROWS), P(ROWS), P(ROWS)),
        out_specs=(P(FEAT, ROWS, None, None), P()),
        check_vma=False,
    )
```

```python
import jax
import jax.numpy as jnp
from jax import lax
from jax.experimental import pallas as pl
from jax.experimental.pallas import tpu as pltpu
from jax.sharding import Mesh
from jax.sharding import PartitionSpec as P

f32, bf16 = jnp.float32, jnp.bfloat16
MESH = pl.DeviceIdType.MESH
BITS = ("z2", "z1", "z0", "y2", "y1", "y0", "xl", "xh", "co")
ROWS, FEAT = BITS[:7], BITS[7:]
CUBE = ("z0", "y0", "xl")
CUBES = [(), ("xl",), ("y0",), ("z0",), ("y0", "xl"), ("z0", "xl"), ("z0", "y0"), ("z0", "y0", "xl")]
PASSES = ((10, 15, 14, 11, 8, 2, 9, 6), (7, 13, 5, 12, 3, 4, 1, 0))
LINES = (("co", "xh", "xl"), ("y2", "y1", "y0"), ("z2", "z1", "z0"))
ROUNDS = (("z2", "z1", "z0", "co"), ("y2", "y1", "y0", "xh", "xl"))
FIRST = (0, 15)
META = 128
MSG = (176, 128)
reg_lambda = 1.0


def ring(e):
    z, y = (((), ("z1",), ("z2", "z0"), ("z2", "z1"))[e // 4], ((), ("y1",), ("y2", "y0"), ("y2", "y1"))[e % 4])
    return z + y


def subset(axes, index):
    return tuple(a for i, a in enumerate(axes) if index >> (len(axes) - 1 - i) & 1)


def peer(flips):
    return {a: 1 - lax.axis_index(a) for a in flips}


def column(flips):
    j = 0
    for a in ROWS:
        b = lax.axis_index(a)
        j = 2 * j + (1 - b if a in flips else b)
    return j


def row(ref, slot, r):
    return jnp.broadcast_to(ref[slot, r:r + 1, :], (16, 128)).astype(bf16)


def side(ref, slot, fs, qs, n, vals, row16):
    zero = jnp.zeros((), bf16)
    cols = []
    for k, q in enumerate(qs):
        rows = []
        for f in fs:
            key = row(ref, slot, f * 16 + q)
            masks = [key == row16 + bf16(16 * i) for i in range(n // 16)]
            for v in vals[k]:
                rows += [jnp.where(m, v, zero) for m in masks]
        cols.append(jnp.concatenate(rows, axis=0))
    return jnp.concatenate(cols, axis=1)


def prep_meta(slot, rbuf, leaff, metaf):
    leaff[slot] = rbuf[slot, META:META + 16, :].astype(f32)
    metaf[slot] = rbuf[slot, META + 16:META + 48, :].astype(f32)


def prep_slot(g, slot, rbuf, lof, hif, leaff):
    leaf = leaff[slot]
    for f in range(8):
        b = rbuf[slot, f * 16:(f + 1) * 16, :].astype(f32)
        w = 64.0 if f < 4 else 32.0
        hi = jnp.floor(b * (1.0 / w))
        lof[slot, f * 16:(f + 1) * 16, :] = b - w * hi
        hif[slot, f * 16:(f + 1) * 16, :] = hi * 16.0 + leaf


def tiles(slot, lof, hif, metaf, accs):
    row16 = lax.broadcasted_iota(jnp.int32, (16, 128), 0).astype(f32).astype(bf16)
    one = jnp.ones((), bf16)
    stage = [0, 0]

    def tile(mxu, acc, fs, qs, vals, a, b):
        rhs = side(lof, slot, fs, qs, b, vals, row16)
        lhs = side(hif, slot, fs, qs, a, [[one], [one]], row16)
        pltpu.matmul_push_rhs(rhs, stage[mxu], mxu, transpose=True)
        pltpu.matmul_acc_lhs(acc, lhs, stage[mxu])
        stage[mxu] ^= 1

    for qp in range(8):
        qs = (2 * qp, 2 * qp + 1)
        vals = [[row(metaf, slot, q), row(metaf, slot, 16 + q)] for q in qs]
        tile(qp % 2, accs[2 + qp % 2], (4, 5, 6, 7), qs, vals, 128, 32)
        for fp in range(2):
            tile(fp, accs[fp], (2 * fp, 2 * fp + 1), qs, vals, 64, 64)


def halves(v, side):
    part = v[:, side * 64:(side + 1) * 64]
    return jnp.concatenate([part[:32], part[32:]], axis=1)


def pop_hists(accs, hs, es, hg, hb, hold=False, more=False):
    def put(e, v):
        if more:
            v = hs[e] + v
        if hold:
            hs[e] = v
            return
        hg[e] = halves(v, 0)
        h = halves(v, 1)
        if e:
            hb[e] = h.astype(bf16)
        else:
            hs[0, 0:32, :] = h

    for fp in range(2):
        r = pltpu.matmul_pop(accs[fp])
        put(es[2 * fp], r[:64, :128])
        put(es[2 * fp + 1], r[64:, 128:])
    both = pltpu.matmul_pop(accs[2]) + pltpu.matmul_pop(accs[3])
    for f in range(4):
        r = both[f * 128:(f + 1) * 128, f * 64:(f + 1) * 64]
        parts = []
        for h in range(4):
            e, o = r[32 * h:32 * h + 16], r[32 * h + 16:32 * h + 32]
            parts.append(jnp.concatenate([e[:, :32], o[:, :32], e[:, 32:], o[:, 32:]], axis=1))
        put(es[4 + f], jnp.concatenate(parts, axis=0))


def prefix_over_lo(h, acc):
    r = lax.broadcasted_iota(jnp.int32, (256, 256), 0) & 127
    c = lax.broadcasted_iota(jnp.int32, (256, 256), 1)
    ones = jnp.where(((r < 64) & (c < 64) & (r <= c)) | ((r >= 64) & (c >= 64) & (c < 128) & (r <= c)), 1.0, 0.0).astype(bf16)
    pltpu.matmul_push_rhs(ones, 0, 0)
    h1 = h.astype(bf16)
    rest = h - h1.astype(f32)
    h2 = rest.astype(bf16)
    h3 = (rest - h2.astype(f32)).astype(bf16)
    pltpu.matmul_acc_lhs(acc, jnp.concatenate([h1, h2], axis=1), 0)
    pltpu.matmul_acc_lhs(acc, jnp.concatenate([h3, jnp.zeros_like(h3)], axis=1), None)
    return pltpu.matmul_pop(acc)[:, :128]


def left_sums(p):
    outs = []
    for v in range(2):
        offset = jnp.zeros((16, 1), f32)
        parts = []
        for hi in range(4):
            block = p[hi * 16:(hi + 1) * 16, v * 64:(v + 1) * 64]
            parts.append(block + offset)
            offset = offset + block[:, 63:64]
        outs.append(jnp.concatenate(parts, axis=1))
    return outs


def gain_of(left_grad, left_hess):
    total_grad = left_grad[:, 255:256]
    total_hess = left_hess[:, 255:256]
    right_grad = total_grad - left_grad
    right_hess = total_hess - left_hess
    return 0.5 * (
        left_grad * left_grad / (left_hess + reg_lambda)
        + right_grad * right_grad / (right_hess + reg_lambda)
        - total_grad * total_grad / (total_hess + reg_lambda)
    )


def kernel(bins_hbm, leaf_hbm, grad_hbm, hess_hbm, gains, best, bins, leaf, grad, hess, tbuf, sbuf0, sbuf1, rbuf0, rbuf1,
           lof, hif, leaff, metaf, hs, hg, hb, rg, rb, mine, theirs,
           in_sem, row_send, row_recv, part_send, part_recv, max_send, max_recv, relay_sem):
    loads = [pltpu.make_async_copy(bins_hbm.at[pl.ds(i * 1024, 1024)], bins.at[pl.ds(i * 1024, 1024)], in_sem.at[i]) for i in range(2)]
    loads += [pltpu.make_async_copy(a, b, in_sem.at[2 + i])
              for i, (a, b) in enumerate(((leaf_hbm, leaf), (grad_hbm, grad), (hess_hbm, hess)))]
    for load in loads:
        load.start()
    partners = set(CUBES[1:]) | {subset(axes, m) for axes in LINES for m in range(1, 8)}
    partners = sorted({tuple(sorted(p)) for p in partners})
    relays = [ring(e) for e in range(1, 4)] + [("co",)] + [subset(("xh", "xl"), m) for m in range(1, 4)]
    barrier = pltpu.get_barrier_semaphore()
    for p in partners:
        pl.semaphore_signal(barrier, inc=1, device_id=peer(p), device_id_type=MESH)

    for q in range(16):
        if q % 8 == 0:
            loads[q // 8].wait()
        tbuf[pl.ds(q, 128, stride=16), :] = bins[q * 128:(q + 1) * 128, :].astype(f32).T
    for load in loads[2:]:
        load.wait()
    meta = [leaf[...].astype(f32).astype(bf16), grad[...], hess[...]]
    sbufs, rbufs = (sbuf0, sbuf1), (rbuf0, rbuf1)

    def pack(g, c):
        buf = sbufs[g] if c else rbufs[g]
        for i, e in enumerate(PASSES[g]):
            j = column(set(CUBES[c]) ^ set(ring(e)))
            buf[c, i * 16:(i + 1) * 16, :] = tbuf[pl.ds(pl.multiple_of(j * 16, 16), 16), :].astype(bf16)
        if g == 0:
            for i, m in enumerate(meta):
                buf[c, META + 16 * i:META + 16 * (i + 1), :] = m

    def row_copy(g, c, flips):
        return pltpu.make_async_remote_copy(
            src_ref=sbufs[g].at[c], dst_ref=rbufs[g].at[c], send_sem=row_send.at[8 * g + c], recv_sem=row_recv.at[8 * g + c],
            device_id=peer(flips), device_id_type=MESH)

    for c in range(1, 8):
        pack(0, c)
    for g in (1, 0):
        pack(g, 0)
    def part_copies(e):
        return [pltpu.make_async_remote_copy(
            src_ref=src.at[e], dst_ref=dst.at[e], send_sem=part_send.at[i, e], recv_sem=part_recv.at[i, e],
            device_id=peer(ring(e)), device_id_type=MESH) for i, (src, dst) in enumerate(((hg, rg), (hb, rb)))]

    def scoped(*accs):
        prep_meta(0, rbuf0, leaff, metaf)
        pl.semaphore_wait(barrier, len(partners))
        for c in range(1, 8):
            row_copy(0, c, CUBES[c]).start()
        for p in relays:
            pl.semaphore_signal(relay_sem, inc=1, device_id=peer(p), device_id_type=MESH)
        prep_slot(1, 0, rbuf1, lof, hif, leaff)
        tiles(0, lof, hif, metaf, accs)
        pop_hists(accs, hs, PASSES[1], hg, hb, hold=True)
        for c in range(1, 8):
            pack(1, c)
        prep_slot(0, 0, rbuf0, lof, hif, leaff)
        tiles(0, lof, hif, metaf, accs)

        def rest(g, slots):
            for c in slots:
                row_copy(g, c, CUBES[c]).wait_recv()
            for c in slots:
                if g == 0:
                    prep_meta(c, rbuf0, leaff, metaf)
                prep_slot(g, c, rbufs[g], lof, hif, leaff)
            for c in slots:
                tiles(c, lof, hif, metaf, accs)

        for c in range(1, 8):
            row_copy(1, c, CUBES[c]).start()
        rest(0, range(1, 4))
        rest(0, range(4, 8))
        for g in range(2):
            if g:
                rest(1, range(1, 4))
                rest(1, range(4, 8))
            pop_hists(accs, hs, PASSES[g], hg, hb, more=g == 1)
            if g == 0:
                pl.semaphore_wait(relay_sem, len(relays))
            for e in PASSES[g]:
                if e:
                    for copy in part_copies(e):
                        copy.start()

        g_sum, h_sum = hg[0], hs[0, 0:32, :]
        for e in PASSES[0] + PASSES[1][:7]:
            for copy in part_copies(e):
                copy.wait_recv()
            g_sum = g_sum + rg[e]
            h_sum = h_sum + rb[e].astype(f32)
        total = jnp.concatenate([
            jnp.concatenate([g_sum[:, :64], h_sum[:, :64]], axis=1), jnp.concatenate([g_sum[:, 64:], h_sum[:, 64:]], axis=1)], axis=0)
        left_grad, left_hess = left_sums(prefix_over_lo(total, accs[4]))
        gain = gain_of(left_grad, left_hess)
        gains[...] = gain
        top = jnp.broadcast_to(jnp.max(gain, axis=1, keepdims=True), (16, 128))
        sub = lax.broadcasted_iota(jnp.int32, (16, 128), 0)
        lane = lax.broadcasted_iota(jnp.int32, (16, 128), 1)
        here = jnp.max(jnp.where(sub == lane, top, -jnp.inf), axis=0, keepdims=True)
        sent = []
        for k, axes in enumerate(ROUNDS):
            mine[k] = here
            steps = range(1, 1 << len(axes))
            copies = [pltpu.make_async_remote_copy(
                src_ref=mine.at[k], dst_ref=theirs.at[FIRST[k] + m - 1], send_sem=max_send.at[FIRST[k] + m - 1],
                recv_sem=max_recv.at[FIRST[k] + m - 1], device_id=peer(subset(axes, m)), device_id_type=MESH) for m in steps]
            for copy in reversed(copies):
                copy.start()
            for copy in copies:
                copy.wait_recv()
            here = jnp.maximum(here, jnp.max(theirs[FIRST[k]:FIRST[k] + len(steps)], axis=0))
            sent += copies
        best[...] = here
        for copy in sent:
            copy.wait_send()

    pl.run_scoped(
        scoped, pltpu.ACC(0)((128, 256), f32), pltpu.ACC(1)((128, 256), f32), pltpu.ACC(0)((512, 256), f32),
        pltpu.ACC(1)((512, 256), f32), pltpu.ACC(0)((64, 256), f32))
    for g in range(2):
        for c in range(1, 8):
            row_copy(g, c, CUBES[c]).wait_send()
    for e in range(1, 16):
        for copy in part_copies(e):
            copy.wait_send()


def body(bin_index, leaf_ids, gradients, hessians):
    vmem = pl.BlockSpec(memory_space=pltpu.VMEM)
    gains, best = pl.pallas_call(
        kernel,
        out_shape=(jax.ShapeDtypeStruct((16, 256), f32), jax.ShapeDtypeStruct((1, 128), f32)),
        in_specs=[pl.BlockSpec(memory_space=pltpu.HBM)] * 4,
        out_specs=(vmem, vmem),
        scratch_shapes=[
            pltpu.VMEM((2048, 128), jnp.int32),
            pltpu.VMEM((16, 128), jnp.int32),
            pltpu.VMEM((16, 128), bf16),
            pltpu.VMEM((16, 128), bf16),
            pltpu.VMEM((2048, 128), f32),
            pltpu.VMEM((8, MSG[0], 128), bf16),
            pltpu.VMEM((8, MSG[1], 128), bf16),
            pltpu.VMEM((8, MSG[0], 128), bf16),
            pltpu.VMEM((8, MSG[1], 128), bf16),
            pltpu.VMEM((8, 128, 128), f32),
            pltpu.VMEM((8, 128, 128), f32),
            pltpu.VMEM((8, 16, 128), f32),
            pltpu.VMEM((8, 32, 128), f32),
            pltpu.VMEM((16, 64, 128), f32),
            pltpu.VMEM((16, 32, 128), f32),
            pltpu.VMEM((16, 32, 128), bf16),
            pltpu.VMEM((16, 32, 128), f32),
            pltpu.VMEM((16, 32, 128), bf16),
            pltpu.VMEM((2, 1, 128), f32),
            pltpu.VMEM((46, 1, 128), f32),
            pltpu.SemaphoreType.DMA((5,)),
            pltpu.SemaphoreType.DMA((16,)),
            pltpu.SemaphoreType.DMA((16,)),
            pltpu.SemaphoreType.DMA((2, 16)),
            pltpu.SemaphoreType.DMA((2, 16)),
            pltpu.SemaphoreType.DMA((46,)),
            pltpu.SemaphoreType.DMA((46,)),
            pltpu.SemaphoreType.REGULAR,
        ],
        compiler_params=pltpu.CompilerParams(collective_id=0, has_side_effects=True, vmem_limit_bytes=48 * 1024 * 1024),
    )(*(pltpu.with_memory_space_constraint(a, pltpu.HBM) for a in (
        bin_index, leaf_ids.reshape(16, 128), gradients.reshape(16, 128), hessians.reshape(16, 128))))
    return gains[None, None], best[0, :LEAVES]


LEAVES = 16


def solution(mesh):
    bits = Mesh(mesh.devices.reshape((2,) * 9), BITS)
    return jax.shard_map(
        body,
        mesh=bits,
        in_specs=(P(ROWS, FEAT), P(ROWS), P(ROWS), P(ROWS)),
        out_specs=(P(FEAT, ROWS, None, None), P()),
        check_vma=False,
    )
```

```python
import jax
import jax.numpy as jnp
from jax import lax
from jax.experimental import pallas as pl
from jax.experimental.pallas import tpu as pltpu
from jax.sharding import Mesh
from jax.sharding import PartitionSpec as P

f32, bf16 = jnp.float32, jnp.bfloat16
MESH = pl.DeviceIdType.MESH
BITS = ("z2", "z1", "z0", "y2", "y1", "y0", "xl", "xh", "co")
ROWS, FEAT = BITS[:7], BITS[7:]
CUBE = ("z0", "y0", "xl")
CUBES = [(), ("xl",), ("y0",), ("z0",), ("y0", "xl"), ("z0", "xl"), ("z0", "y0"), ("z0", "y0", "xl")]
PASSES = ((10, 14, 11, 15, 9, 6, 13, 7), (5, 8, 2, 12, 3, 4, 1, 0))
LINES = (("co", "xh", "xl"), ("y2", "y1", "y0"), ("z2", "z1", "z0"))
ROUNDS = (("z2", "z1", "z0", "co"), ("y2", "y1", "y0", "xh", "xl"))
FIRST = (0, 15)
META = 128
MSG = (176, 128)
reg_lambda = 1.0


def ring(e):
    z, y = (((), ("z1",), ("z2", "z0"), ("z2", "z1"))[e // 4], ((), ("y1",), ("y2", "y0"), ("y2", "y1"))[e % 4])
    return z + y


def subset(axes, index):
    return tuple(a for i, a in enumerate(axes) if index >> (len(axes) - 1 - i) & 1)


def peer(flips):
    return {a: 1 - lax.axis_index(a) for a in flips}


def hops(flips):
    far = {"y2": 4, "y1": 2, "y0": 1, "z2": 4, "z1": 2, "z0": 1, "xh": 2, "xl": 1, "co": 1}
    return sum(far[a] for a in flips if not (a[0] + "2" in flips and a[1] == "1" or a == "xl" and "xh" in flips))


def column(flips):
    j = 0
    for a in ROWS:
        b = lax.axis_index(a)
        j = 2 * j + (1 - b if a in flips else b)
    return j


def row(ref, slot, r):
    return jnp.broadcast_to(ref[slot, r:r + 1, :], (16, 128)).astype(bf16)


def side(ref, slot, fs, qs, n, vals, row16):
    zero = jnp.zeros((), bf16)
    cols = []
    for k, q in enumerate(qs):
        rows = []
        for f in fs:
            key = row(ref, slot, f * 16 + q)
            masks = [key == row16 + bf16(16 * i) for i in range(n // 16)]
            for v in vals[k]:
                rows += [jnp.where(m, v, zero) for m in masks]
        cols.append(jnp.concatenate(rows, axis=0))
    return jnp.concatenate(cols, axis=1)


def prep_meta(slot, rbuf, leaff, metaf):
    leaff[slot] = rbuf[slot, META:META + 16, :].astype(f32)
    metaf[slot] = rbuf[slot, META + 16:META + 48, :].astype(f32)


def prep_slot(g, slot, rbuf, lof, hif, leaff):
    leaf = leaff[slot]
    for f in range(8):
        b = rbuf[slot, f * 16:(f + 1) * 16, :].astype(f32)
        w = 64.0 if f < 4 else 32.0
        hi = jnp.floor(b * (1.0 / w))
        lof[slot, f * 16:(f + 1) * 16, :] = b - w * hi
        hif[slot, f * 16:(f + 1) * 16, :] = hi * 16.0 + leaf


def tiles(slot, lof, hif, metaf, accs):
    row16 = lax.broadcasted_iota(jnp.int32, (16, 128), 0).astype(f32).astype(bf16)
    one = jnp.ones((), bf16)
    stage = [0, 0]

    def tile(mxu, acc, fs, qs, vals, a, b):
        rhs = side(lof, slot, fs, qs, b, vals, row16)
        lhs = side(hif, slot, fs, qs, a, [[one], [one]], row16)
        pltpu.matmul_push_rhs(rhs, stage[mxu], mxu, transpose=True)
        pltpu.matmul_acc_lhs(acc, lhs, stage[mxu])
        stage[mxu] ^= 1

    for qp in range(8):
        qs = (2 * qp, 2 * qp + 1)
        vals = [[row(metaf, slot, q), row(metaf, slot, 16 + q)] for q in qs]
        tile(qp % 2, accs[2 + qp % 2], (4, 5, 6, 7), qs, vals, 128, 32)
        for fp in range(2):
            tile(fp, accs[fp], (2 * fp, 2 * fp + 1), qs, vals, 64, 64)


def pop_hists(accs, hs, es, more=False):
    def put(e, v):
        hs[e] = hs[e] + v if more else v

    for fp in range(2):
        r = pltpu.matmul_pop(accs[fp])
        put(es[2 * fp], r[:64, :128])
        put(es[2 * fp + 1], r[64:, 128:])
    both = pltpu.matmul_pop(accs[2]) + pltpu.matmul_pop(accs[3])
    for f in range(4):
        r = both[f * 128:(f + 1) * 128, f * 64:(f + 1) * 64]
        parts = []
        for h in range(4):
            e, o = r[32 * h:32 * h + 16], r[32 * h + 16:32 * h + 32]
            parts.append(jnp.concatenate([e[:, :32], o[:, :32], e[:, 32:], o[:, 32:]], axis=1))
        put(es[4 + f], jnp.concatenate(parts, axis=0))


def prefix_over_lo(h, acc):
    r = lax.broadcasted_iota(jnp.int32, (256, 256), 0) & 127
    c = lax.broadcasted_iota(jnp.int32, (256, 256), 1)
    ones = jnp.where(((r < 64) & (c < 64) & (r <= c)) | ((r >= 64) & (c >= 64) & (c < 128) & (r <= c)), 1.0, 0.0).astype(bf16)
    pltpu.matmul_push_rhs(ones, 0, 0)
    h1 = h.astype(bf16)
    rest = h - h1.astype(f32)
    h2 = rest.astype(bf16)
    h3 = (rest - h2.astype(f32)).astype(bf16)
    pltpu.matmul_acc_lhs(acc, jnp.concatenate([h1, h2], axis=1), 0)
    pltpu.matmul_acc_lhs(acc, jnp.concatenate([h3, jnp.zeros_like(h3)], axis=1), None)
    return pltpu.matmul_pop(acc)[:, :128]


def left_sums(p):
    outs = []
    for v in range(2):
        offset = jnp.zeros((16, 1), f32)
        parts = []
        for hi in range(4):
            block = p[hi * 16:(hi + 1) * 16, v * 64:(v + 1) * 64]
            parts.append(block + offset)
            offset = offset + block[:, 63:64]
        outs.append(jnp.concatenate(parts, axis=1))
    return outs


def gain_of(left_grad, left_hess):
    total_grad = left_grad[:, 255:256]
    total_hess = left_hess[:, 255:256]
    right_grad = total_grad - left_grad
    right_hess = total_hess - left_hess
    return 0.5 * (
        left_grad * left_grad / (left_hess + reg_lambda)
        + right_grad * right_grad / (right_hess + reg_lambda)
        - total_grad * total_grad / (total_hess + reg_lambda)
    )


def kernel(bins_hbm, leaf_hbm, grad_hbm, hess_hbm, gains, best, bins, leaf, grad, hess, tbuf, sbuf0, sbuf1, rbuf0, rbuf1,
           lof, hif, leaff, metaf, hs, rs, mine, theirs,
           in_sem, row_send, row_recv, part_send, part_recv, max_send, max_recv, relay_sem):
    loads = [pltpu.make_async_copy(bins_hbm.at[pl.ds(i * 1024, 1024)], bins.at[pl.ds(i * 1024, 1024)], in_sem.at[i]) for i in range(2)]
    loads += [pltpu.make_async_copy(a, b, in_sem.at[2 + i])
              for i, (a, b) in enumerate(((leaf_hbm, leaf), (grad_hbm, grad), (hess_hbm, hess)))]
    for load in loads:
        load.start()
    partners = set(CUBES[1:]) | {subset(axes, m) for axes in LINES for m in range(1, 8)}
    partners = sorted({tuple(sorted(p)) for p in partners})
    relays = [ring(e) for e in range(1, 4)] + [("co",)] + [subset(("xh", "xl"), m) for m in range(1, 4)]
    barrier = pltpu.get_barrier_semaphore()
    for p in partners:
        pl.semaphore_signal(barrier, inc=1, device_id=peer(p), device_id_type=MESH)

    for q in range(16):
        if q % 8 == 0:
            loads[q // 8].wait()
        tbuf[pl.ds(q, 128, stride=16), :] = bins[q * 128:(q + 1) * 128, :].astype(f32).T
    for load in loads[2:]:
        load.wait()
    meta = [leaf[...].astype(f32).astype(bf16), grad[...], hess[...]]
    sbufs, rbufs = (sbuf0, sbuf1), (rbuf0, rbuf1)

    def pack(g, c):
        buf = sbufs[g] if c else rbufs[g]
        for i, e in enumerate(PASSES[g]):
            j = column(set(CUBES[c]) ^ set(ring(e)))
            buf[c, i * 16:(i + 1) * 16, :] = tbuf[pl.ds(pl.multiple_of(j * 16, 16), 16), :].astype(bf16)
        if g == 0:
            for i, m in enumerate(meta):
                buf[c, META + 16 * i:META + 16 * (i + 1), :] = m

    def row_copy(g, c, flips):
        return pltpu.make_async_remote_copy(
            src_ref=sbufs[g].at[c], dst_ref=rbufs[g].at[c], send_sem=row_send.at[8 * g + c], recv_sem=row_recv.at[8 * g + c],
            device_id=peer(flips), device_id_type=MESH)

    for c in range(1, 8):
        pack(0, c)
    for g in (1, 0):
        pack(g, 0)
    def part_copy(e):
        return pltpu.make_async_remote_copy(
            src_ref=hs.at[e], dst_ref=rs.at[e], send_sem=part_send.at[e], recv_sem=part_recv.at[e],
            device_id=peer(ring(e)), device_id_type=MESH)

    def scoped(*accs):
        prep_meta(0, rbuf0, leaff, metaf)
        pl.semaphore_wait(barrier, len(partners))
        for c in range(1, 8):
            row_copy(0, c, CUBES[c]).start()
        for p in relays:
            pl.semaphore_signal(relay_sem, inc=1, device_id=peer(p), device_id_type=MESH)
        prep_slot(1, 0, rbuf1, lof, hif, leaff)
        tiles(0, lof, hif, metaf, accs)
        pop_hists(accs, hs, PASSES[1])
        for c in range(1, 8):
            pack(1, c)
        prep_slot(0, 0, rbuf0, lof, hif, leaff)
        tiles(0, lof, hif, metaf, accs)

        def rest(g, slots):
            for c in slots:
                row_copy(g, c, CUBES[c]).wait_recv()
            for c in slots:
                if g == 0:
                    prep_meta(c, rbuf0, leaff, metaf)
                prep_slot(g, c, rbufs[g], lof, hif, leaff)
            for c in slots:
                tiles(c, lof, hif, metaf, accs)

        for c in range(1, 8):
            row_copy(1, c, CUBES[c]).start()
        rest(0, range(1, 4))
        rest(0, range(4, 8))
        for g in range(2):
            if g:
                rest(1, range(1, 4))
                rest(1, range(4, 8))
            pop_hists(accs, hs, PASSES[g], more=g == 1)
            if g == 0:
                pl.semaphore_wait(relay_sem, len(relays))
            for e in PASSES[g]:
                if e:
                    part_copy(e).start()

        total = hs[0]
        for e in PASSES[0] + PASSES[1][:7]:
            part_copy(e).wait_recv()
            total = total + rs[e]
        left_grad, left_hess = left_sums(prefix_over_lo(total, accs[4]))
        gain = gain_of(left_grad, left_hess)
        gains[...] = gain
        top = jnp.broadcast_to(jnp.max(gain, axis=1, keepdims=True), (16, 128))
        sub = lax.broadcasted_iota(jnp.int32, (16, 128), 0)
        lane = lax.broadcasted_iota(jnp.int32, (16, 128), 1)
        here = jnp.max(jnp.where(sub == lane, top, -jnp.inf), axis=0, keepdims=True)
        sent = []
        for k, axes in enumerate(ROUNDS):
            mine[k] = here
            steps = range(1, 1 << len(axes))
            copies = [pltpu.make_async_remote_copy(
                src_ref=mine.at[k], dst_ref=theirs.at[FIRST[k] + m - 1], send_sem=max_send.at[FIRST[k] + m - 1],
                recv_sem=max_recv.at[FIRST[k] + m - 1], device_id=peer(subset(axes, m)), device_id_type=MESH) for m in steps]
            for m in sorted(steps, key=lambda m: -hops(subset(axes, m))):
                copies[m - 1].start()
            for copy in copies:
                copy.wait_recv()
            here = jnp.maximum(here, jnp.max(theirs[FIRST[k]:FIRST[k] + len(steps)], axis=0))
            sent += copies
        best[...] = here
        for copy in sent:
            copy.wait_send()

    pl.run_scoped(
        scoped, pltpu.ACC(0)((128, 256), f32), pltpu.ACC(1)((128, 256), f32), pltpu.ACC(0)((512, 256), f32),
        pltpu.ACC(1)((512, 256), f32), pltpu.ACC(0)((64, 256), f32))
    for g in range(2):
        for c in range(1, 8):
            row_copy(g, c, CUBES[c]).wait_send()
    for e in range(1, 16):
        part_copy(e).wait_send()


def body(bin_index, leaf_ids, gradients, hessians):
    vmem = pl.BlockSpec(memory_space=pltpu.VMEM)
    gains, best = pl.pallas_call(
        kernel,
        out_shape=(jax.ShapeDtypeStruct((16, 256), f32), jax.ShapeDtypeStruct((1, 128), f32)),
        in_specs=[pl.BlockSpec(memory_space=pltpu.HBM)] * 4,
        out_specs=(vmem, vmem),
        scratch_shapes=[
            pltpu.VMEM((2048, 128), jnp.int32),
            pltpu.VMEM((16, 128), jnp.int32),
            pltpu.VMEM((16, 128), bf16),
            pltpu.VMEM((16, 128), bf16),
            pltpu.VMEM((2048, 128), f32),
            pltpu.VMEM((8, MSG[0], 128), bf16),
            pltpu.VMEM((8, MSG[1], 128), bf16),
            pltpu.VMEM((8, MSG[0], 128), bf16),
            pltpu.VMEM((8, MSG[1], 128), bf16),
            pltpu.VMEM((8, 128, 128), f32),
            pltpu.VMEM((8, 128, 128), f32),
            pltpu.VMEM((8, 16, 128), f32),
            pltpu.VMEM((8, 32, 128), f32),
            pltpu.VMEM((16, 64, 128), f32),
            pltpu.VMEM((16, 64, 128), f32),
            pltpu.VMEM((2, 1, 128), f32),
            pltpu.VMEM((46, 1, 128), f32),
            pltpu.SemaphoreType.DMA((5,)),
            pltpu.SemaphoreType.DMA((16,)),
            pltpu.SemaphoreType.DMA((16,)),
            pltpu.SemaphoreType.DMA((16,)),
            pltpu.SemaphoreType.DMA((16,)),
            pltpu.SemaphoreType.DMA((46,)),
            pltpu.SemaphoreType.DMA((46,)),
            pltpu.SemaphoreType.REGULAR,
        ],
        compiler_params=pltpu.CompilerParams(collective_id=0, has_side_effects=True, vmem_limit_bytes=48 * 1024 * 1024),
    )(*(pltpu.with_memory_space_constraint(a, pltpu.HBM) for a in (
        bin_index, leaf_ids.reshape(16, 128), gradients.reshape(16, 128), hessians.reshape(16, 128))))
    return gains[None, None], best[0, :LEAVES]


LEAVES = 16


def solution(mesh):
    bits = Mesh(mesh.devices.reshape((2,) * 9), BITS)
    return jax.shard_map(
        body,
        mesh=bits,
        in_specs=(P(ROWS, FEAT), P(ROWS), P(ROWS), P(ROWS)),
        out_specs=(P(FEAT, ROWS, None, None), P()),
        check_vma=False,
    )
```

```python
import jax
import jax.numpy as jnp
from jax import lax
from jax.experimental import pallas as pl
from jax.experimental.pallas import tpu as pltpu
from jax.sharding import Mesh
from jax.sharding import PartitionSpec as P

f32, bf16 = jnp.float32, jnp.bfloat16
MESH = pl.DeviceIdType.MESH
BITS = ("z2", "z1", "z0", "y2", "y1", "y0", "xl", "xh", "co")
ROWS, FEAT = BITS[:7], BITS[7:]
CUBE = ("z0", "y0", "xl")
CUBES = [(), ("xl",), ("y0",), ("z0",), ("y0", "xl"), ("z0", "xl"), ("z0", "y0"), ("z0", "y0", "xl")]
PASSES = ((10, 15, 14, 11, 8, 2, 9, 6), (7, 13, 5, 12, 3, 4, 1, 0))
LINES = (("co", "xh", "xl"), ("y2", "y1", "y0"), ("z2", "z1", "z0"))
ROUNDS = (("z2", "z1", "z0", "co"), ("y2", "y1", "y0", "xh", "xl"))
FIRST = (0, 15)
META = 128
MSG = (176, 128)
reg_lambda = 1.0


def ring(e):
    z, y = (((), ("z1",), ("z2", "z0"), ("z2", "z1"))[e // 4], ((), ("y1",), ("y2", "y0"), ("y2", "y1"))[e % 4])
    return z + y


def subset(axes, index):
    return tuple(a for i, a in enumerate(axes) if index >> (len(axes) - 1 - i) & 1)


def peer(flips):
    return {a: 1 - lax.axis_index(a) for a in flips}


def hops(flips):
    far = {"y2": 4, "y1": 2, "y0": 1, "z2": 4, "z1": 2, "z0": 1, "xh": 2, "xl": 1, "co": 1}
    return sum(far[a] for a in flips if not (a[0] + "2" in flips and a[1] == "1" or a == "xl" and "xh" in flips))


def column(flips):
    j = 0
    for a in ROWS:
        b = lax.axis_index(a)
        j = 2 * j + (1 - b if a in flips else b)
    return j


def row(ref, slot, r):
    return jnp.broadcast_to(ref[slot, r:r + 1, :], (16, 128)).astype(bf16)


def side(ref, slot, fs, qs, n, vals, row16):
    zero = jnp.zeros((), bf16)
    cols = []
    for k, q in enumerate(qs):
        rows = []
        for f in fs:
            key = row(ref, slot, f * 16 + q)
            masks = [key == row16 + bf16(16 * i) for i in range(n // 16)]
            for v in vals[k]:
                rows += [jnp.where(m, v, zero) for m in masks]
        cols.append(jnp.concatenate(rows, axis=0))
    return jnp.concatenate(cols, axis=1)


def prep_meta(slot, rbuf, leaff, metaf):
    leaff[slot] = rbuf[slot, META:META + 16, :].astype(f32)
    metaf[slot] = rbuf[slot, META + 16:META + 48, :].astype(f32)


def prep_slot(g, slot, rbuf, lof, hif, leaff):
    leaf = leaff[slot]
    for f in range(8):
        b = rbuf[slot, f * 16:(f + 1) * 16, :].astype(f32)
        w = 64.0 if f < 4 else 32.0
        hi = jnp.floor(b * (1.0 / w))
        lof[slot, f * 16:(f + 1) * 16, :] = b - w * hi
        hif[slot, f * 16:(f + 1) * 16, :] = hi * 16.0 + leaf


def tiles(slot, lof, hif, metaf, accs):
    row16 = lax.broadcasted_iota(jnp.int32, (16, 128), 0).astype(f32).astype(bf16)
    one = jnp.ones((), bf16)
    stage = [0, 0]

    def tile(mxu, acc, fs, qs, vals, a, b):
        rhs = side(lof, slot, fs, qs, b, vals, row16)
        lhs = side(hif, slot, fs, qs, a, [[one], [one]], row16)
        pltpu.matmul_push_rhs(rhs, stage[mxu], mxu, transpose=True)
        pltpu.matmul_acc_lhs(acc, lhs, stage[mxu])
        stage[mxu] ^= 1

    for qp in range(8):
        qs = (2 * qp, 2 * qp + 1)
        vals = [[row(metaf, slot, q), row(metaf, slot, 16 + q)] for q in qs]
        tile(qp % 2, accs[2 + qp % 2], (4, 5, 6, 7), qs, vals, 128, 32)
        for fp in range(2):
            tile(fp, accs[fp], (2 * fp, 2 * fp + 1), qs, vals, 64, 64)


def pop_hists(accs, hs, es, more=False):
    def put(e, v):
        hs[e] = hs[e] + v if more else v

    for fp in range(2):
        r = pltpu.matmul_pop(accs[fp])
        put(es[2 * fp], r[:64, :128])
        put(es[2 * fp + 1], r[64:, 128:])
    both = pltpu.matmul_pop(accs[2]) + pltpu.matmul_pop(accs[3])
    for f in range(4):
        r = both[f * 128:(f + 1) * 128, f * 64:(f + 1) * 64]
        parts = []
        for h in range(4):
            e, o = r[32 * h:32 * h + 16], r[32 * h + 16:32 * h + 32]
            parts.append(jnp.concatenate([e[:, :32], o[:, :32], e[:, 32:], o[:, 32:]], axis=1))
        put(es[4 + f], jnp.concatenate(parts, axis=0))


def prefix_over_lo(h, acc):
    r = lax.broadcasted_iota(jnp.int32, (256, 256), 0) & 127
    c = lax.broadcasted_iota(jnp.int32, (256, 256), 1)
    ones = jnp.where(((r < 64) & (c < 64) & (r <= c)) | ((r >= 64) & (c >= 64) & (c < 128) & (r <= c)), 1.0, 0.0).astype(bf16)
    pltpu.matmul_push_rhs(ones, 0, 0)
    h1 = h.astype(bf16)
    rest = h - h1.astype(f32)
    h2 = rest.astype(bf16)
    h3 = (rest - h2.astype(f32)).astype(bf16)
    pltpu.matmul_acc_lhs(acc, jnp.concatenate([h1, h2], axis=1), 0)
    pltpu.matmul_acc_lhs(acc, jnp.concatenate([h3, jnp.zeros_like(h3)], axis=1), None)
    return pltpu.matmul_pop(acc)[:, :128]


def left_sums(p):
    outs = []
    for v in range(2):
        offset = jnp.zeros((16, 1), f32)
        parts = []
        for hi in range(4):
            block = p[hi * 16:(hi + 1) * 16, v * 64:(v + 1) * 64]
            parts.append(block + offset)
            offset = offset + block[:, 63:64]
        outs.append(jnp.concatenate(parts, axis=1))
    return outs


def gain_of(left_grad, left_hess):
    total_grad = left_grad[:, 255:256]
    total_hess = left_hess[:, 255:256]
    right_grad = total_grad - left_grad
    right_hess = total_hess - left_hess
    return 0.5 * (
        left_grad * left_grad / (left_hess + reg_lambda)
        + right_grad * right_grad / (right_hess + reg_lambda)
        - total_grad * total_grad / (total_hess + reg_lambda)
    )


def kernel(bins_hbm, leaf_hbm, grad_hbm, hess_hbm, gains, best, bins, leaf, grad, hess, tbuf, sbuf0, sbuf1, rbuf0, rbuf1,
           lof, hif, leaff, metaf, hs, rs, mine, theirs,
           in_sem, row_send, row_recv, part_send, part_recv, max_send, max_recv, relay_sem):
    loads = [pltpu.make_async_copy(bins_hbm.at[pl.ds(i * 1024, 1024)], bins.at[pl.ds(i * 1024, 1024)], in_sem.at[i]) for i in range(2)]
    loads += [pltpu.make_async_copy(a, b, in_sem.at[2 + i])
              for i, (a, b) in enumerate(((leaf_hbm, leaf), (grad_hbm, grad), (hess_hbm, hess)))]
    for load in loads:
        load.start()
    partners = set(CUBES[1:]) | {subset(axes, m) for axes in LINES for m in range(1, 8)}
    partners = sorted({tuple(sorted(p)) for p in partners}, key=lambda p: (-hops(p), p))
    relays = [ring(e) for e in range(1, 4)] + [("co",)] + [subset(("xh", "xl"), m) for m in range(1, 4)]
    barrier = pltpu.get_barrier_semaphore()
    for p in partners:
        pl.semaphore_signal(barrier, inc=1, device_id=peer(p), device_id_type=MESH)

    for q in range(16):
        if q % 8 == 0:
            loads[q // 8].wait()
        tbuf[pl.ds(q, 128, stride=16), :] = bins[q * 128:(q + 1) * 128, :].astype(f32).T
    for load in loads[2:]:
        load.wait()
    meta = [leaf[...].astype(f32).astype(bf16), grad[...], hess[...]]
    sbufs, rbufs = (sbuf0, sbuf1), (rbuf0, rbuf1)

    def pack(g, c):
        buf = sbufs[g] if c else rbufs[g]
        for i, e in enumerate(PASSES[g]):
            j = column(set(CUBES[c]) ^ set(ring(e)))
            buf[c, i * 16:(i + 1) * 16, :] = tbuf[pl.ds(pl.multiple_of(j * 16, 16), 16), :].astype(bf16)
        if g == 0:
            for i, m in enumerate(meta):
                buf[c, META + 16 * i:META + 16 * (i + 1), :] = m

    def row_copy(g, c, flips):
        return pltpu.make_async_remote_copy(
            src_ref=sbufs[g].at[c], dst_ref=rbufs[g].at[c], send_sem=row_send.at[8 * g + c], recv_sem=row_recv.at[8 * g + c],
            device_id=peer(flips), device_id_type=MESH)

    for c in range(1, 8):
        pack(0, c)
    for g in (1, 0):
        pack(g, 0)
    def part_copy(e):
        return pltpu.make_async_remote_copy(
            src_ref=hs.at[e], dst_ref=rs.at[e], send_sem=part_send.at[e], recv_sem=part_recv.at[e],
            device_id=peer(ring(e)), device_id_type=MESH)

    def scoped(*accs):
        prep_meta(0, rbuf0, leaff, metaf)
        pl.semaphore_wait(barrier, len(partners))
        for c in range(1, 8):
            row_copy(0, c, CUBES[c]).start()
        for p in relays:
            pl.semaphore_signal(relay_sem, inc=1, device_id=peer(p), device_id_type=MESH)
        prep_slot(1, 0, rbuf1, lof, hif, leaff)
        tiles(0, lof, hif, metaf, accs)
        pop_hists(accs, hs, PASSES[1])
        for c in range(1, 8):
            pack(1, c)
        prep_slot(0, 0, rbuf0, lof, hif, leaff)
        tiles(0, lof, hif, metaf, accs)

        def rest(g, slots, then=()):
            for c in slots:
                row_copy(g, c, CUBES[c]).wait_recv()
            for c in then:
                row_copy(1, c, CUBES[c]).start()
            for c in slots:
                if g == 0:
                    prep_meta(c, rbuf0, leaff, metaf)
                prep_slot(g, c, rbufs[g], lof, hif, leaff)
            for c in slots:
                tiles(c, lof, hif, metaf, accs)

        rest(0, range(1, 4), then=range(1, 8))
        rest(0, range(4, 8))
        for g in range(2):
            if g:
                rest(1, range(1, 4))
                rest(1, range(4, 8))
            pop_hists(accs, hs, PASSES[g], more=g == 1)
            if g == 0:
                pl.semaphore_wait(relay_sem, len(relays))
            for e in PASSES[g]:
                if e:
                    part_copy(e).start()

        total = hs[0]
        for e in PASSES[0] + PASSES[1][:7]:
            part_copy(e).wait_recv()
            total = total + rs[e]
        left_grad, left_hess = left_sums(prefix_over_lo(total, accs[4]))
        gain = gain_of(left_grad, left_hess)
        gains[...] = gain
        top = jnp.broadcast_to(jnp.max(gain, axis=1, keepdims=True), (16, 128))
        sub = lax.broadcasted_iota(jnp.int32, (16, 128), 0)
        lane = lax.broadcasted_iota(jnp.int32, (16, 128), 1)
        here = jnp.max(jnp.where(sub == lane, top, -jnp.inf), axis=0, keepdims=True)
        sent = []
        for k, axes in enumerate(ROUNDS):
            mine[k] = here
            steps = range(1, 1 << len(axes))
            copies = [pltpu.make_async_remote_copy(
                src_ref=mine.at[k], dst_ref=theirs.at[FIRST[k] + m - 1], send_sem=max_send.at[FIRST[k] + m - 1],
                recv_sem=max_recv.at[FIRST[k] + m - 1], device_id=peer(subset(axes, m)), device_id_type=MESH) for m in steps]
            for copy in reversed(copies):
                copy.start()
            for copy in copies:
                copy.wait_recv()
            here = jnp.maximum(here, jnp.max(theirs[FIRST[k]:FIRST[k] + len(steps)], axis=0))
            sent += copies
        best[...] = here
        for copy in sent:
            copy.wait_send()

    pl.run_scoped(
        scoped, pltpu.ACC(0)((128, 256), f32), pltpu.ACC(1)((128, 256), f32), pltpu.ACC(0)((512, 256), f32),
        pltpu.ACC(1)((512, 256), f32), pltpu.ACC(0)((64, 256), f32))
    for g in range(2):
        for c in range(1, 8):
            row_copy(g, c, CUBES[c]).wait_send()
    for e in range(1, 16):
        part_copy(e).wait_send()


def body(bin_index, leaf_ids, gradients, hessians):
    vmem = pl.BlockSpec(memory_space=pltpu.VMEM)
    gains, best = pl.pallas_call(
        kernel,
        out_shape=(jax.ShapeDtypeStruct((16, 256), f32), jax.ShapeDtypeStruct((1, 128), f32)),
        in_specs=[pl.BlockSpec(memory_space=pltpu.HBM)] * 4,
        out_specs=(vmem, vmem),
        scratch_shapes=[
            pltpu.VMEM((2048, 128), jnp.int32),
            pltpu.VMEM((16, 128), jnp.int32),
            pltpu.VMEM((16, 128), bf16),
            pltpu.VMEM((16, 128), bf16),
            pltpu.VMEM((2048, 128), f32),
            pltpu.VMEM((8, MSG[0], 128), bf16),
            pltpu.VMEM((8, MSG[1], 128), bf16),
            pltpu.VMEM((8, MSG[0], 128), bf16),
            pltpu.VMEM((8, MSG[1], 128), bf16),
            pltpu.VMEM((8, 128, 128), f32),
            pltpu.VMEM((8, 128, 128), f32),
            pltpu.VMEM((8, 16, 128), f32),
            pltpu.VMEM((8, 32, 128), f32),
            pltpu.VMEM((16, 64, 128), f32),
            pltpu.VMEM((16, 64, 128), f32),
            pltpu.VMEM((2, 1, 128), f32),
            pltpu.VMEM((46, 1, 128), f32),
            pltpu.SemaphoreType.DMA((5,)),
            pltpu.SemaphoreType.DMA((16,)),
            pltpu.SemaphoreType.DMA((16,)),
            pltpu.SemaphoreType.DMA((16,)),
            pltpu.SemaphoreType.DMA((16,)),
            pltpu.SemaphoreType.DMA((46,)),
            pltpu.SemaphoreType.DMA((46,)),
            pltpu.SemaphoreType.REGULAR,
        ],
        compiler_params=pltpu.CompilerParams(collective_id=0, has_side_effects=True, vmem_limit_bytes=48 * 1024 * 1024),
    )(*(pltpu.with_memory_space_constraint(a, pltpu.HBM) for a in (
        bin_index, leaf_ids.reshape(16, 128), gradients.reshape(16, 128), hessians.reshape(16, 128))))
    return gains[None, None], best[0, :LEAVES]


LEAVES = 16


def solution(mesh):
    bits = Mesh(mesh.devices.reshape((2,) * 9), BITS)
    return jax.shard_map(
        body,
        mesh=bits,
        in_specs=(P(ROWS, FEAT), P(ROWS), P(ROWS), P(ROWS)),
        out_specs=(P(FEAT, ROWS, None, None), P()),
        check_vma=False,
    )
```
